32 devices in a mesh: dp: 8 (over y, x, core), tensor: 4 (over z).
Axes of the slice: x: 2, y: 2, z: 4, core: 2. Of those that a mesh axis runs over, the one named last changes fastest.
Arguments:
- tokens: bfloat16 [4096, 2304], P(('dp', 'tensor')), may hold values from -6 to 6
- cotangent: bfloat16 [4096, 4096], P('dp', 'tensor'), may hold values from -6 to 6
- pre_gain: float32 [2304], replicated, may hold values from 0.25 to 1.75
- w_query: bfloat16 [2304, 4096], P('dp', 'tensor'), may hold values from -0.375 to 0.375
- key_weight: bfloat16 [2304, 2048], P('dp', 'tensor'), may hold values from -0.375 to 0.375
- value_weight: bfloat16 [2304, 2048], P('dp', 'tensor'), may hold values from -0.125 to 0.125
Outputs:
- attended: bfloat16 [4096, 4096], P('dp', 'tensor')
- grad_tokens: bfloat16 [4096, 2304], P(('dp', 'tensor'))
- grad_query: float32 [2304, 4096], P('dp', 'tensor')
- grad_key: float32 [2304, 2048], P('dp', 'tensor')
- grad_value: float32 [2304, 2048], P('dp', 'tensor')
- grad_pre_gain: float32 [2304], replicated
The draws below stay inside these ranges and needn't reach their ends.
All inputs are finite; a program needn't handle non-finite values.
Results may differ from the reference program's by a relative error of at most 0.019.
The reference program's roundings to bfloat16 on the way count: a program that leaves them out, or rounds other values in their place, can miss the bound.
Values may be sent and summed in bfloat16 or wider, within the bound.
A program may use at most 192 MiB of HBM per device.

```python
import jax
import jax.numpy as jnp
from jax import lax

MODEL_WIDTH = 2304
QUERY_HEADS = 32
KEY_VALUE_HEADS = 16
HEAD_SIZE = 128
TOK_DEV = 128
SEQ_LEN = 64
TOKENS = 4096
N_DP = 8
N_TENSOR = 4


def block_levels(own_key, dims, cuts, least, high):
    level = 1.0
    for dim, parts in cuts:
        heights = jax.random.uniform(jax.random.fold_in(jax.random.fold_in(own_key, 6), dim), (parts,), jnp.float32, least / len(cuts), high / len(cuts))
        level = level * jnp.repeat(jnp.exp(heights), dims[dim] // parts).reshape((-1,) + (1,) * (len(dims) - 1 - dim))
    return level


def bell_draw(rng, shape, spread, reach, cuts=(), kind=jnp.bfloat16):
    factor_of = block_levels(rng, shape, cuts, -0.22, 0.18) if cuts else 1.0
    result = jax.random.normal(rng, shape, jnp.float32) * spread * factor_of
    return jnp.minimum(jnp.maximum(result, -reach), reach).astype(kind)


def setup_inputs(seed: int = 0) -> dict:
    key_list = jax.random.split(jax.random.key(seed), 7)
    tokens = bell_draw(key_list[0], (TOKENS, MODEL_WIDTH), 1.0, 6.0, ((0, 32),))
    cotangent = bell_draw(key_list[1], (TOKENS, QUERY_HEADS * HEAD_SIZE), 1.0, 6.0, ((0, 8), (1, 4)))
    pre_gain = jnp.clip(1.0 + 0.15 * jax.random.normal(key_list[2], (MODEL_WIDTH,), jnp.float32), 0.25, 1.75)
    w_query = bell_draw(key_list[3], (MODEL_WIDTH, QUERY_HEADS * HEAD_SIZE), (MODEL_WIDTH // 9) ** -0.5, 0.375, ((0, 8), (1, 4)))
    key_weight = bell_draw(key_list[4], (MODEL_WIDTH, KEY_VALUE_HEADS * HEAD_SIZE), (MODEL_WIDTH // 9) ** -0.5, 0.375, ((0, 8), (1, 4)))
    value_weight = bell_draw(key_list[5], (MODEL_WIDTH, KEY_VALUE_HEADS * HEAD_SIZE), MODEL_WIDTH ** -0.5, 0.125, ((0, 8), (1, 4)))
    return {"tokens": tokens, "cotangent": cotangent, "pre_gain": pre_gain, "w_query": w_query, "key_weight": key_weight, "value_weight": value_weight}


EPS = 1e-06
CAP = 50.0
BASE = 10000.0
query_scalar = 144.0

def rotary_tables(segment_length, half):
    places = jnp.arange(segment_length, dtype=jnp.float32)[:, None]
    freqs = BASE ** (-jnp.arange(half, dtype=jnp.float32) / half)
    angles = places * freqs[None, :]
    return (jnp.cos(angles)[:, None, :], jnp.sin(angles)[:, None, :])

def rotate(values, cosine_table, sine_table):
    half = values.shape[-1] // 2
    first, second = (values[..., :half], values[..., half:])
    return jnp.concatenate([first * cosine_table - second * sine_table, second * cosine_table + first * sine_table], -1)

def inverse_rotation(values, cosine_table, sine_table):
    half = values.shape[-1] // 2
    first, second = (values[..., :half], values[..., half:])
    return jnp.concatenate([first * cosine_table + second * sine_table, second * cosine_table - first * sine_table], -1)

def attend_forward(query, key, value):
    repeat = query.shape[1] // key.shape[1]
    keys = jnp.repeat(key, repeat, axis=1).astype(jnp.float32)
    values = jnp.repeat(value, repeat, axis=1).astype(jnp.float32)
    factor = query_scalar ** (-0.5)
    raw = jnp.einsum('qhd,khd->hqk', query.astype(jnp.float32), keys) * factor
    bent = jnp.tanh(raw / CAP)
    capped = CAP * bent
    segment_length = query.shape[0]
    causal = jnp.arange(segment_length)[None, :] <= jnp.arange(segment_length)[:, None]
    raised = jnp.where(causal[None], jnp.exp(capped), 0.0)
    weights = raised / lax.optimization_barrier(jnp.sum(raised, -1, keepdims=True))
    probs = weights.astype(jnp.bfloat16)
    attended = jnp.einsum('hqk,khd->qhd', probs.astype(jnp.float32), values).astype(jnp.bfloat16)
    return (attended, weights, probs, bent)

def attend_backward(d_attended, query, key, value, weights, probs, bent):
    repeat = query.shape[1] // key.shape[1]
    keys = jnp.repeat(key, repeat, axis=1).astype(jnp.float32)
    values = jnp.repeat(value, repeat, axis=1).astype(jnp.float32)
    factor = query_scalar ** (-0.5)
    grad_in = d_attended.astype(jnp.float32)
    d_probs = jnp.einsum('qhd,khd->hqk', grad_in, values)
    d_capped = weights * (d_probs - lax.optimization_barrier(jnp.sum(weights * d_probs, -1, keepdims=True)))
    d_scores = (d_capped * (1.0 - bent * bent) * factor).astype(jnp.bfloat16).astype(jnp.float32)
    query_back = jnp.einsum('hqk,khd->qhd', d_scores, keys)
    key_heads = jnp.einsum('hqk,qhd->khd', d_scores, query.astype(jnp.float32))
    value_heads = jnp.einsum('hqk,qhd->khd', probs.astype(jnp.float32), grad_in)
    segment_length, heads, width = query.shape
    key_rotated_back = key_heads.reshape(segment_length, heads // repeat, repeat, width).sum(2)
    value_returned = value_heads.reshape(segment_length, heads // repeat, repeat, width).sum(2)
    return (query_back, key_rotated_back, value_returned)

def reference(tokens, cotangent, pre_gain, w_query, key_weight, value_weight):
    segment_length = TOK_DEV * N_TENSOR
    token_span = SEQ_LEN
    pieces_count = segment_length // token_span
    query_groups = N_TENSOR
    col_query = QUERY_HEADS * HEAD_SIZE // query_groups
    column_key = KEY_VALUE_HEADS * HEAD_SIZE // query_groups
    cosine_table, sine_table = rotary_tables(token_span, HEAD_SIZE // 2)

    def one_block(carry, pieces):
        rows, cot_rows = pieces
        rows_f = rows.astype(jnp.float32)
        inv_one = lax.rsqrt(lax.optimization_barrier(jnp.mean(rows_f * rows_f, -1, keepdims=True)) + EPS)
        unit_one = rows_f * inv_one
        normed_input = (unit_one * pre_gain).astype(jnp.bfloat16)
        query_raw = jnp.dot(normed_input, w_query, preferred_element_type=jnp.float32).reshape(pieces_count, token_span, QUERY_HEADS, HEAD_SIZE)
        key_unrotated = jnp.dot(normed_input, key_weight, preferred_element_type=jnp.float32).reshape(pieces_count, token_span, KEY_VALUE_HEADS, HEAD_SIZE)
        value_projected = jnp.dot(normed_input, value_weight, preferred_element_type=jnp.float32).reshape(pieces_count, token_span, KEY_VALUE_HEADS, HEAD_SIZE)
        query = rotate(query_raw, cosine_table, sine_table).astype(jnp.bfloat16)
        key = rotate(key_unrotated, cosine_table, sine_table).astype(jnp.bfloat16)
        value = value_projected.astype(jnp.bfloat16)
        attended, weights, probs, bent = jax.vmap(attend_forward)(query, key, value)
        attended = attended.reshape(segment_length, QUERY_HEADS * HEAD_SIZE)
        d_attended = cot_rows.reshape(pieces_count, token_span, QUERY_HEADS, HEAD_SIZE)
        query_back, key_rotated_back, value_returned = jax.vmap(attend_backward)(d_attended, query, key, value, weights, probs, bent)
        d_query = inverse_rotation(query_back, cosine_table, sine_table).astype(jnp.bfloat16).reshape(segment_length, QUERY_HEADS * HEAD_SIZE)
        key_gradient = inverse_rotation(key_rotated_back, cosine_table, sine_table).astype(jnp.bfloat16).reshape(segment_length, KEY_VALUE_HEADS * HEAD_SIZE)
        value_gradient = value_returned.astype(jnp.bfloat16).reshape(segment_length, KEY_VALUE_HEADS * HEAD_SIZE)
        query_part = jnp.dot(normed_input.T, d_query, preferred_element_type=jnp.float32)
        key_part = jnp.dot(normed_input.T, key_gradient, preferred_element_type=jnp.float32)
        value_part = jnp.dot(normed_input.T, value_gradient, preferred_element_type=jnp.float32)
        back = jnp.einsum('lgc,dgc->lgd', d_query.reshape(segment_length, query_groups, col_query).astype(jnp.float32), w_query.reshape(MODEL_WIDTH, query_groups, col_query).astype(jnp.float32))
        back = back + jnp.einsum('lgc,dgc->lgd', key_gradient.reshape(segment_length, query_groups, column_key).astype(jnp.float32), key_weight.reshape(MODEL_WIDTH, query_groups, column_key).astype(jnp.float32))
        back = back + jnp.einsum('lgc,dgc->lgd', value_gradient.reshape(segment_length, query_groups, column_key).astype(jnp.float32), value_weight.reshape(MODEL_WIDTH, query_groups, column_key).astype(jnp.float32))
        back = lax.optimization_barrier(back.astype(jnp.bfloat16))
        d_normed = lax.optimization_barrier(jnp.sum(back.astype(jnp.float32), 1))
        pre_part = lax.optimization_barrier(jnp.sum(d_normed * unit_one, 0))
        scaled_in = d_normed * pre_gain
        grad_rows = (inv_one * (scaled_in - unit_one * lax.optimization_barrier(jnp.mean(scaled_in * unit_one, -1, keepdims=True)))).astype(jnp.bfloat16)
        rounded = lax.optimization_barrier(tuple((part.astype(jnp.bfloat16) for part in (query_part, key_part, value_part))))
        sums = tuple((total + part.astype(jnp.float32) for total, part in zip(carry[:3], rounded)))
        carry = sums + (carry[3] + pre_part,)
        return (carry, (attended, grad_rows))
    start_offset = (jnp.zeros((MODEL_WIDTH, QUERY_HEADS * HEAD_SIZE), jnp.float32), jnp.zeros((MODEL_WIDTH, KEY_VALUE_HEADS * HEAD_SIZE), jnp.float32), jnp.zeros((MODEL_WIDTH, KEY_VALUE_HEADS * HEAD_SIZE), jnp.float32), jnp.zeros((MODEL_WIDTH,), jnp.float32))
    pieces = (tokens.reshape(N_DP, segment_length, MODEL_WIDTH), cotangent.reshape(N_DP, segment_length, QUERY_HEADS * HEAD_SIZE))
    totals, (attended, grad_tokens) = lax.scan(one_block, start_offset, pieces)
    return (attended.reshape(N_DP * segment_length, QUERY_HEADS * HEAD_SIZE), grad_tokens.reshape(N_DP * segment_length, MODEL_WIDTH), totals[0], totals[1], totals[2], totals[3])
```

```python
import functools

import jax
import jax.numpy as jnp
from jax import lax
from jax.experimental import pallas as pl
from jax.experimental.pallas import tpu as pltpu
from jax.sharding import PartitionSpec as P

HEAD_SIZE = 128
SEQ_LEN = 64


EPS = 1e-06
CAP = 50.0
BASE = 10000.0
query_scalar = 144.0


def rotary_tables(segment_length, half):
    places = jnp.arange(segment_length, dtype=jnp.float32)[:, None]
    freqs = BASE ** (-jnp.arange(half, dtype=jnp.float32) / half)
    angles = places * freqs[None, :]
    return (jnp.cos(angles)[:, None, :], jnp.sin(angles)[:, None, :])


def rotate(values, cosine_table, sine_table):
    half = values.shape[-1] // 2
    first, second = (values[..., :half], values[..., half:])
    return jnp.concatenate(
        [first * cosine_table - second * sine_table, second * cosine_table + first * sine_table], -1
    )


def inverse_rotation(values, cosine_table, sine_table):
    half = values.shape[-1] // 2
    first, second = (values[..., :half], values[..., half:])
    return jnp.concatenate(
        [first * cosine_table + second * sine_table, second * cosine_table - first * sine_table], -1
    )


def attend_forward(query, key, value):
    repeat = query.shape[1] // key.shape[1]
    keys = jnp.repeat(key, repeat, axis=1)
    values = jnp.repeat(value, repeat, axis=1)
    factor = query_scalar ** (-0.5)
    raw = jnp.einsum("qhd,khd->hqk", query, keys, preferred_element_type=jnp.float32) * factor
    bent = jnp.tanh(raw / CAP)
    capped = CAP * bent
    segment_length = query.shape[0]
    causal = jnp.arange(segment_length)[None, :] <= jnp.arange(segment_length)[:, None]
    raised = jnp.where(causal[None], jnp.exp(capped), 0.0)
    weights = raised / jnp.sum(raised, -1, keepdims=True)
    probs = weights.astype(jnp.bfloat16)
    attended = jnp.einsum("hqk,khd->qhd", probs, values, preferred_element_type=jnp.float32).astype(
        jnp.bfloat16
    )
    return (attended, weights, probs, bent)


def attend_backward(d_attended, query, key, value, weights, probs, bent):
    repeat = query.shape[1] // key.shape[1]
    keys = jnp.repeat(key, repeat, axis=1)
    values = jnp.repeat(value, repeat, axis=1)
    factor = query_scalar ** (-0.5)
    d_probs = jnp.einsum("qhd,khd->hqk", d_attended, values, preferred_element_type=jnp.float32)
    d_capped = weights * (d_probs - jnp.sum(weights * d_probs, -1, keepdims=True))
    d_scores = (d_capped * (1.0 - bent * bent) * factor).astype(jnp.bfloat16)
    query_back = jnp.einsum("hqk,khd->qhd", d_scores, keys, preferred_element_type=jnp.float32)
    key_heads = jnp.einsum("hqk,qhd->khd", d_scores, query, preferred_element_type=jnp.float32)
    value_heads = jnp.einsum("hqk,qhd->khd", probs, d_attended, preferred_element_type=jnp.float32)
    segment_length, heads, width = query.shape
    key_rotated_back = key_heads.reshape(segment_length, heads // repeat, repeat, width).sum(2)
    value_returned = value_heads.reshape(segment_length, heads // repeat, repeat, width).sum(2)
    return (query_back, key_rotated_back, value_returned)


def segment_pass(query, key, value, d_attended):
    attended, weights, probs, bent = attend_forward(query, key, value)
    query_back, key_rotated_back, value_returned = attend_backward(
        d_attended, query, key, value, weights, probs, bent
    )
    return (attended, query_back, key_rotated_back, value_returned)


def per_device(tokens, cotangent, pre_gain, w_query, key_weight, value_weight):
    contract_first = (((0,), (0,)), ((), ()))
    contract_last = (((1,), (1,)), ((), ()))
    rows_f = tokens.astype(jnp.float32)
    inv_one = lax.rsqrt(jnp.mean(rows_f * rows_f, -1, keepdims=True) + EPS)
    unit_one = rows_f * inv_one
    normed_input = (unit_one * pre_gain).astype(jnp.bfloat16)
    gathered = lax.all_gather(normed_input, "tensor", axis=0, tiled=True)
    segment_length = gathered.shape[0]
    token_span = SEQ_LEN
    pieces_count = segment_length // token_span
    heads_query = w_query.shape[1] // HEAD_SIZE
    heads_key = key_weight.shape[1] // HEAD_SIZE
    pieces = (
        lax.all_gather(w_query, "dp", axis=0, tiled=True),
        lax.all_gather(key_weight, "dp", axis=0, tiled=True),
        lax.all_gather(value_weight, "dp", axis=0, tiled=True),
    )
    query_raw, key_unrotated, value_projected = tuple(
        (jnp.dot(gathered, piece, preferred_element_type=jnp.float32) for piece in pieces)
    )
    cosine_table, sine_table = rotary_tables(token_span, HEAD_SIZE // 2)
    query = rotate(
        query_raw.reshape(pieces_count, token_span, heads_query, HEAD_SIZE),
        cosine_table,
        sine_table,
    ).astype(jnp.bfloat16)
    key = rotate(
        key_unrotated.reshape(pieces_count, token_span, heads_key, HEAD_SIZE),
        cosine_table,
        sine_table,
    ).astype(jnp.bfloat16)
    value = value_projected.reshape(pieces_count, token_span, heads_key, HEAD_SIZE).astype(
        jnp.bfloat16
    )
    d_attended = cotangent.reshape(pieces_count, token_span, heads_query, HEAD_SIZE)
    attended, query_back, key_rotated_back, value_returned = jax.vmap(segment_pass)(
        query, key, value, d_attended
    )
    attended_flat = attended.reshape(segment_length, heads_query * HEAD_SIZE)
    d_query = (
        inverse_rotation(query_back, cosine_table, sine_table)
        .astype(jnp.bfloat16)
        .reshape(segment_length, heads_query * HEAD_SIZE)
    )
    key_gradient = (
        inverse_rotation(key_rotated_back, cosine_table, sine_table)
        .astype(jnp.bfloat16)
        .reshape(segment_length, heads_key * HEAD_SIZE)
    )
    value_gradient = value_returned.astype(jnp.bfloat16).reshape(
        segment_length, heads_key * HEAD_SIZE
    )
    back_query, back_key, back_value = (
        lax.all_gather(w_query, "dp", axis=0, tiled=True),
        lax.all_gather(key_weight, "dp", axis=0, tiled=True),
        lax.all_gather(value_weight, "dp", axis=0, tiled=True),
    )
    joined = jnp.concatenate([d_query, key_gradient, value_gradient], 1)
    block = gathered
    grads = lax.psum_scatter(
        lax.dot_general(block, joined, contract_first, preferred_element_type=jnp.float32).astype(
            jnp.bfloat16
        ),
        "dp",
        scatter_dimension=0,
        tiled=True,
    ).astype(jnp.float32)
    width_query = w_query.shape[1]
    width_key = key_weight.shape[1]
    grad_query = grads[:, :width_query]
    grad_key = grads[:, width_query : width_query + width_key]
    grad_value = grads[:, width_query + width_key :]
    total = jnp.zeros((tokens.shape[0] * lax.axis_size("tensor"), gathered.shape[1]), jnp.float32)
    for grad_part, weight in (
        (d_query, back_query),
        (key_gradient, back_key),
        (value_gradient, back_value),
    ):
        block = grad_part
        total = total + lax.dot_general(
            block, weight, contract_last, preferred_element_type=jnp.float32
        )
    d_normed = lax.psum_scatter(
        total.astype(jnp.bfloat16), "tensor", scatter_dimension=0, tiled=True
    ).astype(jnp.float32)
    pre_part = jnp.sum(d_normed * unit_one, 0)
    scaled_in = d_normed * pre_gain
    grad_tokens = (
        inv_one * (scaled_in - unit_one * jnp.mean(scaled_in * unit_one, -1, keepdims=True))
    ).astype(jnp.bfloat16)
    grad_pre = lax.psum(pre_part, ("dp", "tensor"))
    return (attended_flat, grad_tokens, grad_query, grad_key, grad_value, grad_pre)


F32 = jnp.float32
BF16 = jnp.bfloat16
NN = (((1,), (0,)), ((), ()))
NT = (((1,), (1,)), ((), ()))
TN = (((0,), (0,)), ((), ()))


def swap_halves(values):
    half = values.shape[-1] // 2
    return jnp.concatenate([values[:, half:], values[:, :half]], -1)


def whole_kernel(
    dims,
    tok_ref,
    gain_ref,
    own_ref,
    cot_ref,
    cos_ref,
    sin_ref,
    mask_ref,
    att_ref,
    gtok_ref,
    grad_ref,
    gpre_ref,
    x,
    xt,
    w,
    proj,
    dproj,
    g,
    pr,
    cs,
    dr,
    ar,
    dn,
    rb,
    pb1,
    pb2,
    ws,
    wr,
    xs,
    xr,
    gs,
    gr,
    zs,
    zr,
    ps,
    prs,
):
    n_dp, n_t, chunks, rep, hd = dims
    dp = lax.axis_index("dp")
    t = lax.axis_index("tensor")
    rows = tok_ref.shape[0]
    width = tok_ref.shape[1]
    shard = own_ref.shape[1]
    half = shard // 2
    core = lax.rem(dp, 2)
    chip = lax.div(dp, 2)
    mate, px, py = dp ^ 1, dp ^ 2, dp ^ 4

    barrier = pltpu.get_barrier_semaphore()
    for o in range(1, n_dp):
        pl.semaphore_signal(
            barrier, inc=1, device_id=(dp ^ o, t), device_id_type=pl.DeviceIdType.MESH
        )
    for o in range(1, n_t):
        pl.semaphore_signal(
            barrier, inc=1, device_id=(dp, t ^ o), device_id_type=pl.DeviceIdType.MESH
        )
    pl.semaphore_wait(barrier, n_dp + n_t - 2)

    def rdma(src, dst, ssem, rsem, d, z):
        return pltpu.make_async_remote_copy(
            src_ref=src,
            dst_ref=dst,
            send_sem=ssem,
            recv_sem=rsem,
            device_id=(d, z),
            device_id_type=pl.DeviceIdType.MESH,
        )

    def wrow(who, h=None):
        if h is None:
            return pl.ds(pl.multiple_of(who * shard, 16), shard)
        return pl.ds(pl.multiple_of(who * shard + h * half, 16), half)

    def wcopy(kind, j, origin, to, src=None, h=None):
        place = w.at[j, wrow(origin, h)]
        return rdma(place if src is None else src, place, ws.at[kind, j], wr.at[kind, j], to, t)

    for j in range(chunks):
        wcopy(0, j, dp, px, own_ref.at[j]).start()
        wcopy(1, j, dp, py, own_ref.at[j]).start()

    tokens = tok_ref[...].astype(F32)
    inv = lax.rsqrt(jnp.mean(tokens * tokens, -1, keepdims=True) + EPS)
    x[pl.ds(pl.multiple_of(t * rows, rows), rows), :] = (
        (tokens * inv) * gain_ref[...]
    ).astype(BF16)

    def xcopy(way, o, origin, to):
        place = x.at[pl.ds(pl.multiple_of(origin * rows, rows), rows)]
        return rdma(place, place, xs.at[way, o], xr.at[way, o], dp, to)

    @pl.when(t < n_t - 1)
    def _():
        xcopy(0, 0, t, t + 1).start()

    @pl.when(t > 0)
    def _():
        xcopy(1, 0, t, t - 1).start()

    for j in range(chunks):
        wcopy(2, j, dp, mate, own_ref.at[j]).start()
        w[j, wrow(dp), :] = own_ref[j]

    def relay(j):
        wcopy(0, j, px, px).wait_recv()
        wcopy(5, j, px, py, h=0).start()
        wcopy(3, j, px, mate).start()
        wcopy(1, j, py, py).wait_recv()
        wcopy(6, j, py, px, h=1).start()
        wcopy(4, j, py, mate).start()

    def xrelay(o):
        @pl.when(t - o >= 0)
        def _():
            xcopy(0, o - 1, t - o, t).wait_recv()

            @pl.when(t + 1 < n_t)
            def _():
                xcopy(0, o, t - o, t + 1).start()

        @pl.when(t + o < n_t)
        def _():
            xcopy(1, o - 1, t + o, t).wait_recv()

            @pl.when(t > 0)
            def _():
                xcopy(1, o, t + o, t - 1).start()

    def far(j):
        wcopy(5, j, dp ^ 6, py, h=0).wait_recv()
        wcopy(6, j, dp ^ 6, px, h=1).wait_recv()
        wcopy(7, j, dp ^ 6, mate).start()

    relay(0)
    relay(1)
    xrelay(1)
    relay(2)
    relay(3)
    xrelay(2)
    for j in range(chunks):
        far(j)
    xrelay(3)
    for j in range(chunks):
        wcopy(2, j, mate, mate).wait_recv()
        wcopy(3, j, dp ^ 3, mate).wait_recv()
        wcopy(4, j, dp ^ 5, mate).wait_recv()
        wcopy(7, j, dp ^ 7, mate).wait_recv()

    qw = rep * hd
    cw = qw + 2 * hd
    factor = query_scalar ** (-0.5)
    blocks = x.shape[0] // rows

    xt[...] = x[...].T

    def head(j, carry):
        proj[...] = lax.dot_general(x[...], w[j], NN, preferred_element_type=F32)

        def block(r, c2):
            here = pl.ds(pl.multiple_of(r * rows, rows), rows)
            cosv, sinv = cos_ref[...], sin_ref[...]

            def turn(v):
                return v * cosv + swap_halves(v) * sinv

            def unturn(v):
                return v * cosv - swap_halves(v) * sinv

            q = jnp.concatenate(
                [turn(proj[here, i * hd : (i + 1) * hd]).astype(BF16) for i in range(rep)], 0
            )
            k = turn(proj[here, qw : qw + hd]).astype(BF16)
            v = proj[here, qw + hd : cw].astype(BF16)
            cot = jnp.concatenate(
                [cot_ref[j, here, i * hd : (i + 1) * hd] for i in range(rep)], 0
            )
            bent = jnp.tanh(
                lax.dot_general(q, k, NT, preferred_element_type=F32) * factor / CAP
            )
            raised = jnp.exp(CAP * bent) * mask_ref[...]
            weights = raised / jnp.sum(raised, -1, keepdims=True)
            probs = weights.astype(BF16)
            att = lax.dot_general(probs, v, NN, preferred_element_type=F32).astype(BF16)
            d_probs = lax.dot_general(cot, v, NT, preferred_element_type=F32)
            d_capped = weights * (d_probs - jnp.sum(weights * d_probs, -1, keepdims=True))
            ds = (d_capped * (1.0 - bent * bent) * factor).astype(BF16)
            dq = lax.dot_general(ds, k, NN, preferred_element_type=F32)
            dk = lax.dot_general(ds, q, TN, preferred_element_type=F32)
            dv = lax.dot_general(probs, cot, TN, preferred_element_type=F32)
            for i in range(rep):
                part = slice(i * rows, (i + 1) * rows)
                att_ref[j, here, i * hd : (i + 1) * hd] = att[part]
                dproj[j, here, i * hd : (i + 1) * hd] = unturn(dq[part]).astype(BF16)
            dproj[j, here, qw : qw + hd] = unturn(dk).astype(BF16)
            dproj[j, here, qw + hd : cw] = dv.astype(BF16)
            return c2

        lax.fori_loop(0, blocks, block, 0)
        return carry

    lax.fori_loop(0, chunks, head, 0)

    low = t < n_t // 2
    sign = jnp.where(low, 1, -1)
    m = jnp.where(low, t, n_t - 1 - t)
    fwd = jnp.where(low, 0, 1)

    def mirror(b):
        return jnp.where(low, b, n_t - 1 - b)

    def zcopy(way, b, to):
        src = dn.at[pl.ds(pl.multiple_of(b * rows, rows), rows)]
        return rdma(src, rb.at[way, b], zs.at[way, b], zr.at[way, b], dp, to)

    tile = 256

    def back(i, carry):
        b = mirror(n_t - 1 - i)
        here = pl.ds(pl.multiple_of(b * rows, rows), rows)

        def cols(n, c2):
            span = pl.ds(pl.multiple_of(n * tile, tile), tile)
            total = jnp.zeros((rows, tile), F32)
            for j in range(chunks):
                total += lax.dot_general(
                    dproj[j, here, :], w[j, span, :], NT, preferred_element_type=F32
                )
            dn[here, span] = total.astype(BF16)
            return c2

        lax.fori_loop(0, width // tile, cols, 0)

        @pl.when((m == 0) & (i < n_t - 1))
        def _():
            zcopy(fwd, b, t + sign).start()

        return carry

    lax.fori_loop(0, n_t, back, 0)

    def gcopy(kind, j, src, dst, to):
        return rdma(src, dst, gs.at[kind, j], gr.at[kind, j], to, t)

    def to_mate(j):
        return gcopy(0, j, g.at[j, :, 1 - core], pr.at[j], mate)

    lo, hi = pl.ds(0, half), pl.ds(half, half)
    cx, cy, cd = chip ^ 1, chip ^ 2, chip ^ 3

    def d_x(j):
        return gcopy(1, j, cs.at[j, cd, lo], dr.at[j, lo], px)

    def d_y(j):
        return gcopy(2, j, cs.at[j, cd, hi], dr.at[j, hi], py)

    def x_lo(j):
        return gcopy(3, j, cs.at[j, cx, lo], ar.at[0, j, lo], px)

    def x_hi(j):
        return gcopy(4, j, cs.at[j, cx, hi], ar.at[0, j, hi], px)

    def y_lo(j):
        return gcopy(5, j, cs.at[j, cy, lo], ar.at[1, j, lo], py)

    def y_hi(j):
        return gcopy(6, j, cs.at[j, cy, hi], ar.at[1, j, hi], py)

    def add(*parts):
        total = parts[0].astype(F32)
        for part in parts[1:]:
            total = total + part.astype(F32)
        return total.astype(BF16)

    def product(j):
        for c in range(n_dp // 2):
            for k in range(2):
                who = 2 * c + k
                g[j, c, k] = lax.dot_general(
                    xt[who * shard : (who + 1) * shard, :],
                    dproj[j],
                    NN,
                    preferred_element_type=F32,
                ).astype(BF16)

    def on_chip(j):
        to_mate(j).wait_recv()
        for c in range(n_dp // 2):
            cs[j, c] = add(g[j, c, core], pr[j, c])
        d_x(j).start()
        d_y(j).start()
        x_lo(j).start()
        y_hi(j).start()

    def pass_on(j):
        d_x(j).wait_recv()
        cs[j, cy, lo] = add(cs[j, cy, lo], dr[j, lo])
        y_lo(j).start()
        d_y(j).wait_recv()
        cs[j, cx, hi] = add(cs[j, cx, hi], dr[j, hi])
        x_hi(j).start()

    def grads_step(j, carry):
        @pl.when(j < chunks)
        def _():
            product(j)
            to_mate(j).start()

        @pl.when(j > 0)
        def _():
            on_chip(j - 1)

        return carry

    lax.fori_loop(0, chunks + 1, grads_step, 0)

    def zsum(way, b):
        here = pl.ds(pl.multiple_of(b * rows, rows), rows)
        zcopy(way, b, t).wait_recv()
        dn[here, :] = add(dn[here, :], rb[way, b])

    @pl.when(m > 0)
    def _():
        b = mirror(n_t - 1)
        zsum(fwd, b)
        zcopy(fwd, b, t + sign).start()

    pass_on(0)
    pass_on(1)

    @pl.when(m > 0)
    def _():
        b = mirror(0)
        zsum(1 - fwd, b)
        zcopy(1 - fwd, b, t - sign).start()
        b2 = mirror(n_t - 2)
        zsum(fwd, b2)
        zcopy(fwd, b2, t + sign).start()

    pass_on(2)
    pass_on(3)

    mine = pl.ds(pl.multiple_of(t * rows, rows), rows)
    zcopy(1 - fwd, t, t).wait_recv()

    @pl.when(m > 0)
    def _():
        zcopy(fwd, t, t).wait_recv()

    @pl.when(m == 0)
    def _():
        rb[fwd, t] = jnp.zeros((rows, width), BF16)

    d_normed = dn[mine, :].astype(F32) + rb[0, t].astype(F32) + rb[1, t].astype(F32)
    tokens2 = tok_ref[...].astype(F32)
    inv2 = lax.rsqrt(jnp.mean(tokens2 * tokens2, -1, keepdims=True) + EPS)
    unit = tokens2 * inv2
    pb1[dp] = jnp.sum(d_normed * unit, 0, keepdims=True)

    def p1(o):
        return rdma(pb1.at[dp], pb1.at[dp], ps.at[0, o], prs.at[0, o], dp ^ o, t)

    def p2(o):
        return rdma(pb2.at[t], pb2.at[t], ps.at[1, o], prs.at[1, o], dp, t ^ o)

    def p1r(o):
        return rdma(pb1.at[dp ^ o], pb1.at[dp ^ o], ps.at[0, o], prs.at[0, o], dp ^ o, t)

    def p2r(o):
        return rdma(pb2.at[t ^ o], pb2.at[t ^ o], ps.at[1, o], prs.at[1, o], dp, t ^ o)

    for o in range(1, n_dp):
        p1(o).start()
    e = d_normed * gain_ref[...]
    gtok_ref[...] = (inv2 * (e - unit * jnp.mean(e * unit, -1, keepdims=True))).astype(BF16)
    for o in range(1, n_dp):
        p1r(o).wait_recv()
    total = pb1[0]
    for o in range(1, n_dp):
        total = total + pb1[o]
    pb2[t] = total
    for o in range(1, n_t):
        p2(o).start()

    for j in range(chunks):
        x_lo(j).wait_recv()
        y_hi(j).wait_recv()
        y_lo(j).wait_recv()
        x_hi(j).wait_recv()
        grad_ref[j] = add(cs[j, chip], ar[0, j], ar[1, j])

    for o in range(1, n_t):
        p2r(o).wait_recv()
    total = pb2[0]
    for o in range(1, n_t):
        total = total + pb2[o]
    gpre_ref[...] = total

    for j in range(chunks):
        wcopy(0, j, dp, px, own_ref.at[j]).wait_send()
        wcopy(1, j, dp, py, own_ref.at[j]).wait_send()
        wcopy(2, j, dp, mate, own_ref.at[j]).wait_send()
        wcopy(3, j, px, mate).wait_send()
        wcopy(4, j, py, mate).wait_send()
        wcopy(5, j, px, py, h=0).wait_send()
        wcopy(6, j, py, px, h=1).wait_send()
        wcopy(7, j, dp ^ 6, mate).wait_send()
        to_mate(j).wait_send()
        for copy in (d_x, d_y, x_lo, x_hi, y_lo, y_hi):
            copy(j).wait_send()
    for o in range(n_t - 1):
        @pl.when((t - o >= 0) & (t + 1 < n_t))
        def _():
            xcopy(0, o, t - o, t + 1).wait_send()

        @pl.when((t + o < n_t) & (t > 0))
        def _():
            xcopy(1, o, t + o, t - 1).wait_send()

    for b in range(n_t - 1, 0, -1):
        @pl.when(m < b)
        def _():
            zcopy(fwd, mirror(b), t + sign).wait_send()

    @pl.when(m > 0)
    def _():
        zcopy(1 - fwd, mirror(0), t - sign).wait_send()

    for o in range(1, n_dp):
        p1(o).wait_send()
    for o in range(1, n_t):
        p2(o).wait_send()


def fused_per_device(tokens, cotangent, pre_gain, w_query, key_weight, value_weight):
    n_dp, n_t = lax.axis_size("dp"), lax.axis_size("tensor")
    rows, width = tokens.shape
    block = rows * n_t
    shard = w_query.shape[0]
    chunks = key_weight.shape[1] // HEAD_SIZE
    rep = w_query.shape[1] // key_weight.shape[1]
    qw = rep * HEAD_SIZE
    cw = qw + 2 * HEAD_SIZE
    parts = (
        w_query.reshape(shard, chunks, qw),
        key_weight.reshape(shard, chunks, HEAD_SIZE),
        value_weight.reshape(shard, chunks, HEAD_SIZE),
    )
    own = jnp.concatenate(parts, -1).transpose(1, 0, 2)
    cot = cotangent.reshape(block, chunks, qw).transpose(1, 0, 2)
    cosine, sine = rotary_tables(SEQ_LEN, HEAD_SIZE // 2)
    reps = rows // SEQ_LEN
    cosine = jnp.tile(jnp.concatenate([cosine[:, 0], cosine[:, 0]], -1), (reps, 1))
    sine = jnp.tile(jnp.concatenate([-sine[:, 0], sine[:, 0]], -1), (reps, 1))
    place = jnp.arange(rows)
    mask = (place[None, :] <= place[:, None]) & (
        place[None, :] // SEQ_LEN == place[:, None] // SEQ_LEN
    )
    mask = jnp.tile(mask.astype(F32), (rep, 1))
    vmem = pl.BlockSpec(memory_space=pltpu.VMEM)
    dma = pltpu.SemaphoreType.DMA
    att, grad_tokens, grads, grad_pre = pl.pallas_call(
        functools.partial(whole_kernel, (n_dp, n_t, chunks, rep, HEAD_SIZE)),
        out_shape=(
            jax.ShapeDtypeStruct((chunks, block, qw), BF16),
            jax.ShapeDtypeStruct((rows, width), BF16),
            jax.ShapeDtypeStruct((chunks, shard, cw), BF16),
            jax.ShapeDtypeStruct((1, width), F32),
        ),
        in_specs=[vmem] * 7,
        out_specs=(vmem,) * 4,
        scratch_shapes=[
            pltpu.VMEM((block, width), BF16),
            pltpu.VMEM((width, block), BF16),
            pltpu.VMEM((chunks, width, cw), BF16),
            pltpu.VMEM((block, cw), F32),
            pltpu.VMEM((chunks, block, cw), BF16),
            pltpu.VMEM((chunks, n_dp // 2, 2, shard, cw), BF16),
            pltpu.VMEM((chunks, n_dp // 2, shard, cw), BF16),
            pltpu.VMEM((chunks, n_dp // 2, shard, cw), BF16),
            pltpu.VMEM((chunks, shard, cw), BF16),
            pltpu.VMEM((2, chunks, shard, cw), BF16),
            pltpu.VMEM((block, width), BF16),
            pltpu.VMEM((2, n_t, rows, width), BF16),
            pltpu.VMEM((n_dp, 1, width), F32),
            pltpu.VMEM((n_t, 1, width), F32),
            dma((8, chunks)),
            dma((8, chunks)),
            dma((2, n_t)),
            dma((2, n_t)),
            dma((7, chunks)),
            dma((7, chunks)),
            dma((2, n_t)),
            dma((2, n_t)),
            dma((2, n_dp)),
            dma((2, n_dp)),
        ],
        compiler_params=pltpu.CompilerParams(
            collective_id=0, has_side_effects=True, vmem_limit_bytes=62 * 1024 * 1024
        ),
    )(tokens, pre_gain[None, :], own, cot, cosine, sine, mask)
    attended = att.transpose(1, 0, 2).reshape(block, chunks * qw)
    grads = grads.astype(F32)
    grad_query = grads[:, :, :qw].transpose(1, 0, 2).reshape(shard, chunks * qw)
    grad_key = grads[:, :, qw : qw + HEAD_SIZE].transpose(1, 0, 2)
    grad_value = grads[:, :, qw + HEAD_SIZE :].transpose(1, 0, 2)
    return (
        attended,
        grad_tokens,
        grad_query,
        grad_key.reshape(shard, chunks * HEAD_SIZE),
        grad_value.reshape(shard, chunks * HEAD_SIZE),
        grad_pre[0],
    )


def solution(mesh):
    fused = mesh.shape["dp"] == 8 and mesh.shape["tensor"] == 4
    placed = (
        P(("dp", "tensor"), None),
        P("dp", "tensor"),
        P(),
        P("dp", "tensor"),
        P("dp", "tensor"),
        P("dp", "tensor"),
    )
    return jax.shard_map(
        fused_per_device if fused else per_device,
        mesh=mesh,
        in_specs=placed,
        out_specs=(
            P("dp", "tensor"),
            P(("dp", "tensor"), None),
            P("dp", "tensor"),
            P("dp", "tensor"),
            P("dp", "tensor"),
            P(),
        ),
        check_vma=False,
    )
```

```python
import functools

import jax
import jax.numpy as jnp
import numpy as np
from jax import lax
from jax.experimental import pallas as pl
from jax.experimental.pallas import tpu as pltpu
from jax.sharding import PartitionSpec as P

HEAD_SIZE = 128
SEQ_LEN = 64


EPS = 1e-06
CAP = 50.0
BASE = 10000.0
query_scalar = 144.0


def rotary_tables(segment_length, half):
    places = jnp.arange(segment_length, dtype=jnp.float32)[:, None]
    freqs = BASE ** (-jnp.arange(half, dtype=jnp.float32) / half)
    angles = places * freqs[None, :]
    return (jnp.cos(angles)[:, None, :], jnp.sin(angles)[:, None, :])


def rotate(values, cosine_table, sine_table):
    half = values.shape[-1] // 2
    first, second = (values[..., :half], values[..., half:])
    return jnp.concatenate(
        [first * cosine_table - second * sine_table, second * cosine_table + first * sine_table], -1
    )


def inverse_rotation(values, cosine_table, sine_table):
    half = values.shape[-1] // 2
    first, second = (values[..., :half], values[..., half:])
    return jnp.concatenate(
        [first * cosine_table + second * sine_table, second * cosine_table - first * sine_table], -1
    )


def attend_forward(query, key, value):
    repeat = query.shape[1] // key.shape[1]
    keys = jnp.repeat(key, repeat, axis=1)
    values = jnp.repeat(value, repeat, axis=1)
    factor = query_scalar ** (-0.5)
    raw = jnp.einsum("qhd,khd->hqk", query, keys, preferred_element_type=jnp.float32) * factor
    bent = jnp.tanh(raw / CAP)
    capped = CAP * bent
    segment_length = query.shape[0]
    causal = jnp.arange(segment_length)[None, :] <= jnp.arange(segment_length)[:, None]
    raised = jnp.where(causal[None], jnp.exp(capped), 0.0)
    weights = raised / jnp.sum(raised, -1, keepdims=True)
    probs = weights.astype(jnp.bfloat16)
    attended = jnp.einsum("hqk,khd->qhd", probs, values, preferred_element_type=jnp.float32).astype(
        jnp.bfloat16
    )
    return (attended, weights, probs, bent)


def attend_backward(d_attended, query, key, value, weights, probs, bent):
    repeat = query.shape[1] // key.shape[1]
    keys = jnp.repeat(key, repeat, axis=1)
    values = jnp.repeat(value, repeat, axis=1)
    factor = query_scalar ** (-0.5)
    d_probs = jnp.einsum("qhd,khd->hqk", d_attended, values, preferred_element_type=jnp.float32)
    d_capped = weights * (d_probs - jnp.sum(weights * d_probs, -1, keepdims=True))
    d_scores = (d_capped * (1.0 - bent * bent) * factor).astype(jnp.bfloat16)
    query_back = jnp.einsum("hqk,khd->qhd", d_scores, keys, preferred_element_type=jnp.float32)
    key_heads = jnp.einsum("hqk,qhd->khd", d_scores, query, preferred_element_type=jnp.float32)
    value_heads = jnp.einsum("hqk,qhd->khd", probs, d_attended, preferred_element_type=jnp.float32)
    segment_length, heads, width = query.shape
    key_rotated_back = key_heads.reshape(segment_length, heads // repeat, repeat, width).sum(2)
    value_returned = value_heads.reshape(segment_length, heads // repeat, repeat, width).sum(2)
    return (query_back, key_rotated_back, value_returned)


def segment_pass(query, key, value, d_attended):
    attended, weights, probs, bent = attend_forward(query, key, value)
    query_back, key_rotated_back, value_returned = attend_backward(
        d_attended, query, key, value, weights, probs, bent
    )
    return (attended, query_back, key_rotated_back, value_returned)


def per_device(tokens, cotangent, pre_gain, w_query, key_weight, value_weight):
    contract_first = (((0,), (0,)), ((), ()))
    contract_last = (((1,), (1,)), ((), ()))
    rows_f = tokens.astype(jnp.float32)
    inv_one = lax.rsqrt(jnp.mean(rows_f * rows_f, -1, keepdims=True) + EPS)
    unit_one = rows_f * inv_one
    normed_input = (unit_one * pre_gain).astype(jnp.bfloat16)
    gathered = lax.all_gather(normed_input, "tensor", axis=0, tiled=True)
    segment_length = gathered.shape[0]
    token_span = SEQ_LEN
    pieces_count = segment_length // token_span
    heads_query = w_query.shape[1] // HEAD_SIZE
    heads_key = key_weight.shape[1] // HEAD_SIZE
    pieces = (
        lax.all_gather(w_query, "dp", axis=0, tiled=True),
        lax.all_gather(key_weight, "dp", axis=0, tiled=True),
        lax.all_gather(value_weight, "dp", axis=0, tiled=True),
    )
    query_raw, key_unrotated, value_projected = tuple(
        (jnp.dot(gathered, piece, preferred_element_type=jnp.float32) for piece in pieces)
    )
    cosine_table, sine_table = rotary_tables(token_span, HEAD_SIZE // 2)
    query = rotate(
        query_raw.reshape(pieces_count, token_span, heads_query, HEAD_SIZE),
        cosine_table,
        sine_table,
    ).astype(jnp.bfloat16)
    key = rotate(
        key_unrotated.reshape(pieces_count, token_span, heads_key, HEAD_SIZE),
        cosine_table,
        sine_table,
    ).astype(jnp.bfloat16)
    value = value_projected.reshape(pieces_count, token_span, heads_key, HEAD_SIZE).astype(
        jnp.bfloat16
    )
    d_attended = cotangent.reshape(pieces_count, token_span, heads_query, HEAD_SIZE)
    attended, query_back, key_rotated_back, value_returned = jax.vmap(segment_pass)(
        query, key, value, d_attended
    )
    attended_flat = attended.reshape(segment_length, heads_query * HEAD_SIZE)
    d_query = (
        inverse_rotation(query_back, cosine_table, sine_table)
        .astype(jnp.bfloat16)
        .reshape(segment_length, heads_query * HEAD_SIZE)
    )
    key_gradient = (
        inverse_rotation(key_rotated_back, cosine_table, sine_table)
        .astype(jnp.bfloat16)
        .reshape(segment_length, heads_key * HEAD_SIZE)
    )
    value_gradient = value_returned.astype(jnp.bfloat16).reshape(
        segment_length, heads_key * HEAD_SIZE
    )
    back_query, back_key, back_value = (
        lax.all_gather(w_query, "dp", axis=0, tiled=True),
        lax.all_gather(key_weight, "dp", axis=0, tiled=True),
        lax.all_gather(value_weight, "dp", axis=0, tiled=True),
    )
    joined = jnp.concatenate([d_query, key_gradient, value_gradient], 1)
    block = gathered
    grads = lax.psum_scatter(
        lax.dot_general(block, joined, contract_first, preferred_element_type=jnp.float32).astype(
            jnp.bfloat16
        ),
        "dp",
        scatter_dimension=0,
        tiled=True,
    ).astype(jnp.float32)
    width_query = w_query.shape[1]
    width_key = key_weight.shape[1]
    grad_query = grads[:, :width_query]
    grad_key = grads[:, width_query : width_query + width_key]
    grad_value = grads[:, width_query + width_key :]
    total = jnp.zeros((tokens.shape[0] * lax.axis_size("tensor"), gathered.shape[1]), jnp.float32)
    for grad_part, weight in (
        (d_query, back_query),
        (key_gradient, back_key),
        (value_gradient, back_value),
    ):
        block = grad_part
        total = total + lax.dot_general(
            block, weight, contract_last, preferred_element_type=jnp.float32
        )
    d_normed = lax.psum_scatter(
        total.astype(jnp.bfloat16), "tensor", scatter_dimension=0, tiled=True
    ).astype(jnp.float32)
    pre_part = jnp.sum(d_normed * unit_one, 0)
    scaled_in = d_normed * pre_gain
    grad_tokens = (
        inv_one * (scaled_in - unit_one * jnp.mean(scaled_in * unit_one, -1, keepdims=True))
    ).astype(jnp.bfloat16)
    grad_pre = lax.psum(pre_part, ("dp", "tensor"))
    return (attended_flat, grad_tokens, grad_query, grad_key, grad_value, grad_pre)


F32 = jnp.float32
BF16 = jnp.bfloat16
NN = (((1,), (0,)), ((), ()))
NT = (((1,), (1,)), ((), ()))
TN = (((0,), (0,)), ((), ()))


def swap_halves(values):
    half = values.shape[-1] // 2
    return jnp.concatenate([values[:, half:], values[:, :half]], -1)


def whole_kernel(
    dims,
    tok_ref,
    gain_ref,
    wq_ref,
    wk_ref,
    wv_ref,
    cot_ref,
    cos_ref,
    sin_ref,
    mask_ref,
    att_ref,
    gtok_ref,
    gq_ref,
    gk_ref,
    gv_ref,
    gpre_ref,
    x,
    xt,
    w,
    proj,
    dproj,
    g,
    pr,
    cs,
    dr,
    ar,
    dn,
    rb,
    pb1,
    pb2,
    ws,
    wr,
    xs,
    xr,
    gs,
    gr,
    zs,
    zr,
    ps,
    prs,
    ls,
):
    n_dp, n_t, chunks, rep, hd = dims
    dp = lax.axis_index("dp")
    t = lax.axis_index("tensor")
    rows = tok_ref.shape[0]
    width = tok_ref.shape[1]
    shard = wq_ref.shape[0]
    qw = rep * hd
    cw = qw + 2 * hd
    half = shard // 2
    core = lax.rem(dp, 2)
    chip = lax.div(dp, 2)
    mate, px, py = dp ^ 1, dp ^ 2, dp ^ 4

    def own_copies(j):
        here = pl.ds(pl.multiple_of(dp * shard, 16), shard)
        return (
            pltpu.make_async_copy(
                wq_ref.at[:, j * qw : (j + 1) * qw], w.at[j, here, 0:qw], ls.at[0, j]
            ),
            pltpu.make_async_copy(
                wk_ref.at[:, j * hd : (j + 1) * hd], w.at[j, here, qw : qw + hd], ls.at[1, j]
            ),
            pltpu.make_async_copy(
                wv_ref.at[:, j * hd : (j + 1) * hd], w.at[j, here, qw + hd : cw], ls.at[2, j]
            ),
        )

    for j in range(chunks):
        for copy in own_copies(j):
            copy.start()

    barrier = pltpu.get_barrier_semaphore()
    for o in range(1, n_dp):
        pl.semaphore_signal(
            barrier, inc=1, device_id=(dp ^ o, t), device_id_type=pl.DeviceIdType.MESH
        )
    for o in range(1, n_t):
        pl.semaphore_signal(
            barrier, inc=1, device_id=(dp, t ^ o), device_id_type=pl.DeviceIdType.MESH
        )
    pl.semaphore_wait(barrier, n_dp + n_t - 2)

    def rdma(src, dst, ssem, rsem, d, z):
        return pltpu.make_async_remote_copy(
            src_ref=src,
            dst_ref=dst,
            send_sem=ssem,
            recv_sem=rsem,
            device_id=(d, z),
            device_id_type=pl.DeviceIdType.MESH,
        )

    def wrow(who, h=None):
        if h is None:
            return pl.ds(pl.multiple_of(who * shard, 16), shard)
        return pl.ds(pl.multiple_of(who * shard + h * half, 16), half)

    def wcopy(kind, j, origin, to, h=None):
        place = w.at[j, wrow(origin, h)]
        return rdma(place, place, ws.at[kind, j], wr.at[kind, j], to, t)

    def offer(j):
        wcopy(0, j, dp, px).start()
        wcopy(1, j, dp, py).start()

    for j in range(chunks):
        for copy in own_copies(j):
            copy.wait()
        if j < 2:
            offer(j)

    tokens = tok_ref[...].astype(F32)
    inv = lax.rsqrt(jnp.mean(tokens * tokens, -1, keepdims=True) + EPS)
    x[pl.ds(pl.multiple_of(t * rows, rows), rows), :] = (
        (tokens * inv) * gain_ref[...][None, :]
    ).astype(BF16)

    def xcopy(way, o, origin, to):
        place = x.at[pl.ds(pl.multiple_of(origin * rows, rows), rows)]
        return rdma(place, place, xs.at[way, o], xr.at[way, o], dp, to)

    @pl.when(t < n_t - 1)
    def _():
        xcopy(0, 0, t, t + 1).start()

    @pl.when(t > 0)
    def _():
        xcopy(1, 0, t, t - 1).start()

    for j in range(chunks):
        wcopy(2, j, dp, mate).start()

    def relay(j):
        wcopy(0, j, px, px).wait_recv()
        wcopy(5, j, px, py, h=0).start()
        wcopy(3, j, px, mate).start()
        wcopy(1, j, py, py).wait_recv()
        wcopy(6, j, py, px, h=1).start()
        wcopy(4, j, py, mate).start()

    def xrelay(o):
        @pl.when(t - o >= 0)
        def _():
            xcopy(0, o - 1, t - o, t).wait_recv()

            @pl.when(t + 1 < n_t)
            def _():
                xcopy(0, o, t - o, t + 1).start()

        @pl.when(t + o < n_t)
        def _():
            xcopy(1, o - 1, t + o, t).wait_recv()

            @pl.when(t > 0)
            def _():
                xcopy(1, o, t + o, t - 1).start()

    def far(j):
        wcopy(5, j, dp ^ 6, py, h=0).wait_recv()
        wcopy(6, j, dp ^ 6, px, h=1).wait_recv()
        wcopy(7, j, dp ^ 6, mate).start()

    def ready(j):
        far(j)
        wcopy(2, j, mate, mate).wait_recv()
        wcopy(3, j, dp ^ 3, mate).wait_recv()
        wcopy(4, j, dp ^ 5, mate).wait_recv()
        wcopy(7, j, dp ^ 7, mate).wait_recv()

    factor = query_scalar ** (-0.5)
    low = t < n_t // 2
    sign = jnp.where(low, 1, -1)
    m = jnp.where(low, t, n_t - 1 - t)
    fwd = jnp.where(low, 0, 1)

    def mirror(b):
        return jnp.where(low, b, n_t - 1 - b)

    places = (
        t,
        jnp.where(m == 0, t + sign, t - sign),
        jnp.where(m == 0, t + 2 * sign, t + sign),
        mirror(n_t - 1),
    )

    def head_cols(j, i):
        return pl.ds(pl.multiple_of(j * qw + i * hd, hd), hd)

    def tiles(*which):
        for slot, (j, p) in enumerate(which):
            here = pl.ds(pl.multiple_of(places[p] * rows, rows), rows)
            proj[slot] = lax.dot_general(x[here, :], w[j], NN, preferred_element_type=F32)
        for slot, (j, p) in enumerate(which):
            here = pl.ds(pl.multiple_of(places[p] * rows, rows), rows)
            cosv, sinv = cos_ref[...], sin_ref[...]

            def turn(v):
                return v * cosv + swap_halves(v) * sinv

            def unturn(v):
                return v * cosv - swap_halves(v) * sinv

            q = jnp.concatenate(
                [turn(proj[slot, :, i * hd : (i + 1) * hd]).astype(BF16) for i in range(rep)], 0
            )
            k = turn(proj[slot, :, qw : qw + hd]).astype(BF16)
            v = proj[slot, :, qw + hd : cw].astype(BF16)
            cot = jnp.concatenate(
                [cot_ref[here, head_cols(j, i)] for i in range(rep)], 0
            )
            bent = jnp.tanh(
                lax.dot_general(q, k, NT, preferred_element_type=F32) * factor / CAP
            )
            raised = jnp.exp(CAP * bent) * mask_ref[...]
            weights = raised / jnp.sum(raised, -1, keepdims=True)
            probs = weights.astype(BF16)
            att = lax.dot_general(probs, v, NN, preferred_element_type=F32).astype(BF16)
            d_probs = lax.dot_general(cot, v, NT, preferred_element_type=F32)
            d_capped = weights * (d_probs - jnp.sum(weights * d_probs, -1, keepdims=True))
            ds = (d_capped * (1.0 - bent * bent) * factor).astype(BF16)
            dq = lax.dot_general(ds, k, NN, preferred_element_type=F32)
            dk = lax.dot_general(ds, q, TN, preferred_element_type=F32)
            dv = lax.dot_general(probs, cot, TN, preferred_element_type=F32)
            for i in range(rep):
                part = slice(i * rows, (i + 1) * rows)
                att_ref[here, head_cols(j, i)] = att[part]
                dproj[j, here, i * hd : (i + 1) * hd] = unturn(dq[part]).astype(BF16)
            dproj[j, here, qw : qw + hd] = unturn(dk).astype(BF16)
            dproj[j, here, qw + hd : cw] = dv.astype(BF16)
    def zcopy(way, b, to):
        src = dn.at[pl.ds(pl.multiple_of(b * rows, rows), rows)]
        return rdma(src, rb.at[way, b], zs.at[way, b], zr.at[way, b], dp, to)

    tile = 256

    def back(first, count):
        here = pl.ds(pl.multiple_of(first * rows, rows), count * rows)

        def cols(n, c2):
            span = pl.ds(pl.multiple_of(n * tile, tile), tile)
            total = lax.dot_general(
                dproj[0, here, :], w[0, span, :], NT, preferred_element_type=F32
            )
            for j in range(1, chunks):
                total += lax.dot_general(
                    dproj[j, here, :], w[j, span, :], NT, preferred_element_type=F32
                )
            dn[here, span] = total.astype(BF16)
            return c2

        lax.fori_loop(0, width // tile, cols, 0)

    def outward(b):
        zcopy(fwd, mirror(b), t + sign).start()

    def gcopy(kind, j, src, dst, to):
        return rdma(src, dst, gs.at[kind, j], gr.at[kind, j], to, t)

    def to_mate(j):
        return gcopy(0, j, g.at[j, :, 1 - core], pr.at[j], mate)

    lo, hi = pl.ds(0, half), pl.ds(half, half)
    cx, cy, cd = chip ^ 1, chip ^ 2, chip ^ 3

    def d_x(j):
        return gcopy(1, j, cs.at[j, cd, lo], dr.at[j, lo], px)

    def d_y(j):
        return gcopy(2, j, cs.at[j, cd, hi], dr.at[j, hi], py)

    def x_lo(j):
        return gcopy(3, j, cs.at[j, cx, lo], ar.at[0, j, lo], px)

    def x_hi(j):
        return gcopy(4, j, cs.at[j, cx, hi], ar.at[0, j, hi], px)

    def y_lo(j):
        return gcopy(5, j, cs.at[j, cy, lo], ar.at[1, j, lo], py)

    def y_hi(j):
        return gcopy(6, j, cs.at[j, cy, hi], ar.at[1, j, hi], py)

    def add(*parts):
        total = parts[0].astype(F32)
        for part in parts[1:]:
            total = total + part.astype(F32)
        return total.astype(BF16)

    def product(j):
        def share(c, c2):
            for k in range(2):
                span = pl.ds(pl.multiple_of((2 * c + k) * shard, 16), shard)
                g[j, c, k] = lax.dot_general(
                    xt[span, :], dproj[j], NN, preferred_element_type=F32
                ).astype(BF16)
            return c2

        lax.fori_loop(0, n_dp // 2, share, 0)
        to_mate(j).start()

    def on_chip(j):
        to_mate(j).wait_recv()
        for c in range(n_dp // 2):
            cs[j, c] = add(g[j, c, core], pr[j, c])
        d_x(j).start()
        d_y(j).start()
        x_lo(j).start()
        y_hi(j).start()

    def pass_on(j):
        d_x(j).wait_recv()
        cs[j, cy, lo] = add(cs[j, cy, lo], dr[j, lo])
        y_lo(j).start()
        d_y(j).wait_recv()
        cs[j, cx, hi] = add(cs[j, cx, hi], dr[j, hi])
        x_hi(j).start()

    def zsum(way, b):
        here = pl.ds(pl.multiple_of(b * rows, rows), rows)
        zcopy(way, b, t).wait_recv()
        dn[here, :] = add(dn[here, :], rb[way, b])

    far_block = mirror(n_t - 1)
    rest = jnp.where(low, 0, 1)

    relay(0)
    offer(2)
    relay(1)
    offer(3)
    xrelay(1)
    ready(0)
    tiles((0, 0), (0, 1))
    relay(2)
    ready(1)
    xrelay(2)
    tiles((1, 0), (1, 1))
    tiles((0, 2), (1, 2))
    relay(3)
    ready(2)
    tiles((2, 0), (2, 1), (2, 2))
    ready(3)
    xrelay(3)
    tiles((0, 3), (1, 3))
    xt[...] = x[...].T
    product(0)
    tiles((2, 3), (3, 3))
    back(far_block, 1)

    @pl.when(m == 0)
    def _():
        outward(n_t - 1)

    on_chip(0)
    product(1)
    tiles((3, 0), (3, 1), (3, 2))
    back(rest, n_t - 1)

    @pl.when(m == 0)
    def _():
        outward(n_t - 2)
        outward(1)

    on_chip(1)
    product(2)

    @pl.when(m > 0)
    def _():
        zsum(fwd, far_block)
        outward(n_t - 1)

    product(3)
    on_chip(2)
    pass_on(0)
    on_chip(3)
    pass_on(1)

    @pl.when(m > 0)
    def _():
        b = mirror(0)
        zsum(1 - fwd, b)
        zcopy(1 - fwd, b, t - sign).start()
        zsum(fwd, mirror(n_t - 2))
        outward(n_t - 2)

    pass_on(2)
    pass_on(3)

    mine = pl.ds(pl.multiple_of(t * rows, rows), rows)
    zcopy(1 - fwd, t, t).wait_recv()

    @pl.when(m > 0)
    def _():
        zcopy(fwd, t, t).wait_recv()

    @pl.when(m == 0)
    def _():
        rb[fwd, t] = jnp.zeros((rows, width), BF16)

    d_normed = dn[mine, :].astype(F32) + rb[0, t].astype(F32) + rb[1, t].astype(F32)
    tokens2 = tok_ref[...].astype(F32)
    inv2 = lax.rsqrt(jnp.mean(tokens2 * tokens2, -1, keepdims=True) + EPS)
    unit = tokens2 * inv2
    pb1[dp] = jnp.sum(d_normed * unit, 0, keepdims=True)

    def p1(o):
        return rdma(pb1.at[dp], pb1.at[dp], ps.at[0, o], prs.at[0, o], dp ^ o, t)

    def p2(o):
        return rdma(pb2.at[t], pb2.at[t], ps.at[1, o], prs.at[1, o], dp, t ^ o)

    def p1r(o):
        return rdma(pb1.at[dp ^ o], pb1.at[dp ^ o], ps.at[0, o], prs.at[0, o], dp ^ o, t)

    def p2r(o):
        return rdma(pb2.at[t ^ o], pb2.at[t ^ o], ps.at[1, o], prs.at[1, o], dp, t ^ o)

    for o in range(1, n_dp):
        p1(o).start()
    e = d_normed * gain_ref[...][None, :]
    gtok_ref[...] = (inv2 * (e - unit * jnp.mean(e * unit, -1, keepdims=True))).astype(BF16)
    for o in range(1, n_dp):
        p1r(o).wait_recv()
    total = pb1[0]
    for o in range(1, n_dp):
        total = total + pb1[o]
    pb2[t] = total
    for o in range(1, n_t):
        p2(o).start()

    for j in range(chunks):
        x_lo(j).wait_recv()
        y_hi(j).wait_recv()
        y_lo(j).wait_recv()
        x_hi(j).wait_recv()
        done = add(cs[j, chip], ar[0, j], ar[1, j])
        gq_ref[:, j * qw : (j + 1) * qw] = done[:, :qw]
        gk_ref[:, j * hd : (j + 1) * hd] = done[:, qw : qw + hd]
        gv_ref[:, j * hd : (j + 1) * hd] = done[:, qw + hd :]

    for o in range(1, n_t):
        p2r(o).wait_recv()
    total = pb2[0]
    for o in range(1, n_t):
        total = total + pb2[o]
    gpre_ref[...] = total[0]

    for j in range(chunks):
        wcopy(0, j, dp, px).wait_send()
        wcopy(1, j, dp, py).wait_send()
        wcopy(2, j, dp, mate).wait_send()
        wcopy(3, j, px, mate).wait_send()
        wcopy(4, j, py, mate).wait_send()
        wcopy(5, j, px, py, h=0).wait_send()
        wcopy(6, j, py, px, h=1).wait_send()
        wcopy(7, j, dp ^ 6, mate).wait_send()
        to_mate(j).wait_send()
        for copy in (d_x, d_y, x_lo, x_hi, y_lo, y_hi):
            copy(j).wait_send()
    for o in range(n_t - 1):
        @pl.when((t - o >= 0) & (t + 1 < n_t))
        def _():
            xcopy(0, o, t - o, t + 1).wait_send()

        @pl.when((t + o < n_t) & (t > 0))
        def _():
            xcopy(1, o, t + o, t - 1).wait_send()

    for b in range(n_t - 1, 0, -1):
        @pl.when(m < b)
        def _():
            zcopy(fwd, mirror(b), t + sign).wait_send()

    @pl.when(m > 0)
    def _():
        zcopy(1 - fwd, mirror(0), t - sign).wait_send()

    for o in range(1, n_dp):
        p1(o).wait_send()
    for o in range(1, n_t):
        p2(o).wait_send()


def fused_per_device(tokens, cotangent, pre_gain, w_query, key_weight, value_weight):
    n_dp, n_t = lax.axis_size("dp"), lax.axis_size("tensor")
    rows, width = tokens.shape
    block = rows * n_t
    shard = w_query.shape[0]
    chunks = key_weight.shape[1] // HEAD_SIZE
    rep = w_query.shape[1] // key_weight.shape[1]
    qw = rep * HEAD_SIZE
    cw = qw + 2 * HEAD_SIZE
    half = HEAD_SIZE // 2
    place = np.arange(rows)
    freqs = BASE ** (-np.arange(half) / half)
    angles = (place % SEQ_LEN)[:, None] * freqs[None, :]
    cosine = np.concatenate([np.cos(angles)] * 2, -1).astype(np.float32)
    sine = np.concatenate([-np.sin(angles), np.sin(angles)], -1).astype(np.float32)
    mask = (place[None, :] <= place[:, None]) & (
        place[None, :] // SEQ_LEN == place[:, None] // SEQ_LEN
    )
    mask = np.tile(mask.astype(np.float32), (rep, 1))
    vmem = pl.BlockSpec(memory_space=pltpu.VMEM)
    hbm = pl.BlockSpec(memory_space=pl.ANY)
    dma = pltpu.SemaphoreType.DMA
    attended, grad_tokens, gq, gk, gv, grad_pre = pl.pallas_call(
        functools.partial(whole_kernel, (n_dp, n_t, chunks, rep, HEAD_SIZE)),
        out_shape=(
            jax.ShapeDtypeStruct((block, chunks * qw), BF16),
            jax.ShapeDtypeStruct((rows, width), BF16),
            jax.ShapeDtypeStruct((shard, chunks * qw), BF16),
            jax.ShapeDtypeStruct((shard, chunks * HEAD_SIZE), BF16),
            jax.ShapeDtypeStruct((shard, chunks * HEAD_SIZE), BF16),
            jax.ShapeDtypeStruct((width,), F32),
        ),
        in_specs=[vmem, vmem, hbm, hbm, hbm] + [vmem] * 4,
        out_specs=(vmem,) * 6,
        scratch_shapes=[
            pltpu.VMEM((block, width), BF16),
            pltpu.VMEM((width, block), BF16),
            pltpu.VMEM((chunks, width, cw), BF16),
            pltpu.VMEM((3, rows, cw), F32),
            pltpu.VMEM((chunks, block, cw), BF16),
            pltpu.VMEM((chunks, n_dp // 2, 2, shard, cw), BF16),
            pltpu.VMEM((chunks, n_dp // 2, shard, cw), BF16),
            pltpu.VMEM((chunks, n_dp // 2, shard, cw), BF16),
            pltpu.VMEM((chunks, shard, cw), BF16),
            pltpu.VMEM((2, chunks, shard, cw), BF16),
            pltpu.VMEM((block, width), BF16),
            pltpu.VMEM((2, n_t, rows, width), BF16),
            pltpu.VMEM((n_dp, 1, width), F32),
            pltpu.VMEM((n_t, 1, width), F32),
            dma((8, chunks)),
            dma((8, chunks)),
            dma((2, n_t)),
            dma((2, n_t)),
            dma((7, chunks)),
            dma((7, chunks)),
            dma((2, n_t)),
            dma((2, n_t)),
            dma((2, n_dp)),
            dma((2, n_dp)),
            dma((3, chunks)),
        ],
        compiler_params=pltpu.CompilerParams(
            collective_id=0, has_side_effects=True, vmem_limit_bytes=62 * 1024 * 1024
        ),
    )(tokens, pre_gain, w_query, key_weight, value_weight, cotangent, cosine, sine, mask)
    return (
        attended,
        grad_tokens,
        gq.astype(F32),
        gk.astype(F32),
        gv.astype(F32),
        grad_pre,
    )


def solution(mesh):
    fused = mesh.shape["dp"] == 8 and mesh.shape["tensor"] == 4
    placed = (
        P(("dp", "tensor"), None),
        P("dp", "tensor"),
        P(),
        P("dp", "tensor"),
        P("dp", "tensor"),
        P("dp", "tensor"),
    )
    return jax.shard_map(
        fused_per_device if fused else per_device,
        mesh=mesh,
        in_specs=placed,
        out_specs=(
            P("dp", "tensor"),
            P(("dp", "tensor"), None),
            P("dp", "tensor"),
            P("dp", "tensor"),
            P("dp", "tensor"),
            P(),
        ),
        check_vma=False,
    )
```

```python
import functools

import jax
import jax.numpy as jnp
import numpy as np
from jax import lax
from jax.experimental import pallas as pl
from jax.experimental.pallas import tpu as pltpu
from jax.sharding import PartitionSpec as P

HEAD_SIZE = 128
SEQ_LEN = 64


EPS = 1e-06
CAP = 50.0
BASE = 10000.0
query_scalar = 144.0


def rotary_tables(segment_length, half):
    places = jnp.arange(segment_length, dtype=jnp.float32)[:, None]
    freqs = BASE ** (-jnp.arange(half, dtype=jnp.float32) / half)
    angles = places * freqs[None, :]
    return (jnp.cos(angles)[:, None, :], jnp.sin(angles)[:, None, :])


def rotate(values, cosine_table, sine_table):
    half = values.shape[-1] // 2
    first, second = (values[..., :half], values[..., half:])
    return jnp.concatenate(
        [first * cosine_table - second * sine_table, second * cosine_table + first * sine_table], -1
    )


def inverse_rotation(values, cosine_table, sine_table):
    half = values.shape[-1] // 2
    first, second = (values[..., :half], values[..., half:])
    return jnp.concatenate(
        [first * cosine_table + second * sine_table, second * cosine_table - first * sine_table], -1
    )


def attend_forward(query, key, value):
    repeat = query.shape[1] // key.shape[1]
    keys = jnp.repeat(key, repeat, axis=1)
    values = jnp.repeat(value, repeat, axis=1)
    factor = query_scalar ** (-0.5)
    raw = jnp.einsum("qhd,khd->hqk", query, keys, preferred_element_type=jnp.float32) * factor
    bent = jnp.tanh(raw / CAP)
    capped = CAP * bent
    segment_length = query.shape[0]
    causal = jnp.arange(segment_length)[None, :] <= jnp.arange(segment_length)[:, None]
    raised = jnp.where(causal[None], jnp.exp(capped), 0.0)
    weights = raised / jnp.sum(raised, -1, keepdims=True)
    probs = weights.astype(jnp.bfloat16)
    attended = jnp.einsum("hqk,khd->qhd", probs, values, preferred_element_type=jnp.float32).astype(
        jnp.bfloat16
    )
    return (attended, weights, probs, bent)


def attend_backward(d_attended, query, key, value, weights, probs, bent):
    repeat = query.shape[1] // key.shape[1]
    keys = jnp.repeat(key, repeat, axis=1)
    values = jnp.repeat(value, repeat, axis=1)
    factor = query_scalar ** (-0.5)
    d_probs = jnp.einsum("qhd,khd->hqk", d_attended, values, preferred_element_type=jnp.float32)
    d_capped = weights * (d_probs - jnp.sum(weights * d_probs, -1, keepdims=True))
    d_scores = (d_capped * (1.0 - bent * bent) * factor).astype(jnp.bfloat16)
    query_back = jnp.einsum("hqk,khd->qhd", d_scores, keys, preferred_element_type=jnp.float32)
    key_heads = jnp.einsum("hqk,qhd->khd", d_scores, query, preferred_element_type=jnp.float32)
    value_heads = jnp.einsum("hqk,qhd->khd", probs, d_attended, preferred_element_type=jnp.float32)
    segment_length, heads, width = query.shape
    key_rotated_back = key_heads.reshape(segment_length, heads // repeat, repeat, width).sum(2)
    value_returned = value_heads.reshape(segment_length, heads // repeat, repeat, width).sum(2)
    return (query_back, key_rotated_back, value_returned)


def segment_pass(query, key, value, d_attended):
    attended, weights, probs, bent = attend_forward(query, key, value)
    query_back, key_rotated_back, value_returned = attend_backward(
        d_attended, query, key, value, weights, probs, bent
    )
    return (attended, query_back, key_rotated_back, value_returned)


def per_device(tokens, cotangent, pre_gain, w_query, key_weight, value_weight):
    contract_first = (((0,), (0,)), ((), ()))
    contract_last = (((1,), (1,)), ((), ()))
    rows_f = tokens.astype(jnp.float32)
    inv_one = lax.rsqrt(jnp.mean(rows_f * rows_f, -1, keepdims=True) + EPS)
    unit_one = rows_f * inv_one
    normed_input = (unit_one * pre_gain).astype(jnp.bfloat16)
    gathered = lax.all_gather(normed_input, "tensor", axis=0, tiled=True)
    segment_length = gathered.shape[0]
    token_span = SEQ_LEN
    pieces_count = segment_length // token_span
    heads_query = w_query.shape[1] // HEAD_SIZE
    heads_key = key_weight.shape[1] // HEAD_SIZE
    pieces = (
        lax.all_gather(w_query, "dp", axis=0, tiled=True),
        lax.all_gather(key_weight, "dp", axis=0, tiled=True),
        lax.all_gather(value_weight, "dp", axis=0, tiled=True),
    )
    query_raw, key_unrotated, value_projected = tuple(
        (jnp.dot(gathered, piece, preferred_element_type=jnp.float32) for piece in pieces)
    )
    cosine_table, sine_table = rotary_tables(token_span, HEAD_SIZE // 2)
    query = rotate(
        query_raw.reshape(pieces_count, token_span, heads_query, HEAD_SIZE),
        cosine_table,
        sine_table,
    ).astype(jnp.bfloat16)
    key = rotate(
        key_unrotated.reshape(pieces_count, token_span, heads_key, HEAD_SIZE),
        cosine_table,
        sine_table,
    ).astype(jnp.bfloat16)
    value = value_projected.reshape(pieces_count, token_span, heads_key, HEAD_SIZE).astype(
        jnp.bfloat16
    )
    d_attended = cotangent.reshape(pieces_count, token_span, heads_query, HEAD_SIZE)
    attended, query_back, key_rotated_back, value_returned = jax.vmap(segment_pass)(
        query, key, value, d_attended
    )
    attended_flat = attended.reshape(segment_length, heads_query * HEAD_SIZE)
    d_query = (
        inverse_rotation(query_back, cosine_table, sine_table)
        .astype(jnp.bfloat16)
        .reshape(segment_length, heads_query * HEAD_SIZE)
    )
    key_gradient = (
        inverse_rotation(key_rotated_back, cosine_table, sine_table)
        .astype(jnp.bfloat16)
        .reshape(segment_length, heads_key * HEAD_SIZE)
    )
    value_gradient = value_returned.astype(jnp.bfloat16).reshape(
        segment_length, heads_key * HEAD_SIZE
    )
    back_query, back_key, back_value = (
        lax.all_gather(w_query, "dp", axis=0, tiled=True),
        lax.all_gather(key_weight, "dp", axis=0, tiled=True),
        lax.all_gather(value_weight, "dp", axis=0, tiled=True),
    )
    joined = jnp.concatenate([d_query, key_gradient, value_gradient], 1)
    block = gathered
    grads = lax.psum_scatter(
        lax.dot_general(block, joined, contract_first, preferred_element_type=jnp.float32).astype(
            jnp.bfloat16
        ),
        "dp",
        scatter_dimension=0,
        tiled=True,
    ).astype(jnp.float32)
    width_query = w_query.shape[1]
    width_key = key_weight.shape[1]
    grad_query = grads[:, :width_query]
    grad_key = grads[:, width_query : width_query + width_key]
    grad_value = grads[:, width_query + width_key :]
    total = jnp.zeros((tokens.shape[0] * lax.axis_size("tensor"), gathered.shape[1]), jnp.float32)
    for grad_part, weight in (
        (d_query, back_query),
        (key_gradient, back_key),
        (value_gradient, back_value),
    ):
        block = grad_part
        total = total + lax.dot_general(
            block, weight, contract_last, preferred_element_type=jnp.float32
        )
    d_normed = lax.psum_scatter(
        total.astype(jnp.bfloat16), "tensor", scatter_dimension=0, tiled=True
    ).astype(jnp.float32)
    pre_part = jnp.sum(d_normed * unit_one, 0)
    scaled_in = d_normed * pre_gain
    grad_tokens = (
        inv_one * (scaled_in - unit_one * jnp.mean(scaled_in * unit_one, -1, keepdims=True))
    ).astype(jnp.bfloat16)
    grad_pre = lax.psum(pre_part, ("dp", "tensor"))
    return (attended_flat, grad_tokens, grad_query, grad_key, grad_value, grad_pre)


F32 = jnp.float32
BF16 = jnp.bfloat16
NN = (((1,), (0,)), ((), ()))
NT = (((1,), (1,)), ((), ()))
TN = (((0,), (0,)), ((), ()))


def swap_halves(values):
    half = values.shape[-1] // 2
    return jnp.concatenate([values[:, half:], values[:, :half]], -1)


def whole_kernel(
    dims,
    tok_ref,
    gain_ref,
    wq_ref,
    wk_ref,
    wv_ref,
    cot_ref,
    cos_ref,
    sin_ref,
    mask_ref,
    att_ref,
    gtok_ref,
    gq_ref,
    gk_ref,
    gv_ref,
    gpre_ref,
    x,
    xt,
    w,
    proj,
    dproj,
    g,
    pr,
    cs,
    dr,
    ar,
    dn,
    rb,
    pb1,
    pb2,
    ws,
    wr,
    xs,
    xr,
    gs,
    gr,
    zs,
    zr,
    ps,
    prs,
    ls,
):
    n_dp, n_t, chunks, rep, hd = dims
    dp = lax.axis_index("dp")
    t = lax.axis_index("tensor")
    rows = tok_ref.shape[0]
    width = tok_ref.shape[1]
    shard = wq_ref.shape[0]
    qw = rep * hd
    cw = qw + 2 * hd
    half = shard // 2
    core = lax.rem(dp, 2)
    chip = lax.div(dp, 2)
    mate, px, py = dp ^ 1, dp ^ 2, dp ^ 4

    def own_copies(j):
        here = pl.ds(pl.multiple_of(dp * shard, 16), shard)
        return (
            pltpu.make_async_copy(
                wq_ref.at[:, j * qw : (j + 1) * qw], w.at[j, here, 0:qw], ls.at[0, j]
            ),
            pltpu.make_async_copy(
                wk_ref.at[:, j * hd : (j + 1) * hd], w.at[j, here, qw : qw + hd], ls.at[1, j]
            ),
            pltpu.make_async_copy(
                wv_ref.at[:, j * hd : (j + 1) * hd], w.at[j, here, qw + hd : cw], ls.at[2, j]
            ),
        )

    for j in range(chunks):
        for copy in own_copies(j):
            copy.start()

    barrier = pltpu.get_barrier_semaphore()
    for o in range(1, n_dp):
        pl.semaphore_signal(
            barrier, inc=1, device_id=(dp ^ o, t), device_id_type=pl.DeviceIdType.MESH
        )
    for o in range(1, n_t):
        pl.semaphore_signal(
            barrier, inc=1, device_id=(dp, t ^ o), device_id_type=pl.DeviceIdType.MESH
        )
    pl.semaphore_wait(barrier, n_dp + n_t - 2)

    def rdma(src, dst, ssem, rsem, d, z):
        return pltpu.make_async_remote_copy(
            src_ref=src,
            dst_ref=dst,
            send_sem=ssem,
            recv_sem=rsem,
            device_id=(d, z),
            device_id_type=pl.DeviceIdType.MESH,
        )

    def wrow(who, h=None):
        if h is None:
            return pl.ds(pl.multiple_of(who * shard, 16), shard)
        return pl.ds(pl.multiple_of(who * shard + h * half, 16), half)

    def wcopy(kind, j, origin, to, h=None):
        place = w.at[j, wrow(origin, h)]
        return rdma(place, place, ws.at[kind, j], wr.at[kind, j], to, t)

    def offer(j):
        wcopy(0, j, dp, px).start()
        wcopy(1, j, dp, py).start()

    for j in range(chunks):
        for copy in own_copies(j):
            copy.wait()
        if j < 2:
            offer(j)

    tokens = tok_ref[...].astype(F32)
    inv = lax.rsqrt(jnp.mean(tokens * tokens, -1, keepdims=True) + EPS)
    x[pl.ds(pl.multiple_of(t * rows, rows), rows), :] = (
        (tokens * inv) * gain_ref[...][None, :]
    ).astype(BF16)

    piece = rows // 2

    def xcopy(way, o, h, origin, to):
        place = x.at[pl.ds(pl.multiple_of(origin * rows + h * piece, piece), piece)]
        return rdma(place, place, xs.at[way, o, h], xr.at[way, o, h], dp, to)

    @pl.when(t < n_t - 1)
    def _():
        for h in range(2):
            xcopy(0, 0, h, t, t + 1).start()

    @pl.when(t > 0)
    def _():
        for h in range(2):
            xcopy(1, 0, h, t, t - 1).start()

    for j in range(chunks):
        wcopy(2, j, dp, mate).start()

    def relay(j):
        wcopy(0, j, px, px).wait_recv()
        wcopy(5, j, px, py, h=0).start()
        wcopy(3, j, px, mate).start()
        wcopy(1, j, py, py).wait_recv()
        wcopy(6, j, py, px, h=1).start()
        wcopy(4, j, py, mate).start()

    def xrelay(o, h):
        @pl.when(t - o >= 0)
        def _():
            xcopy(0, o - 1, h, t - o, t).wait_recv()

            @pl.when(t + 1 < n_t)
            def _():
                xcopy(0, o, h, t - o, t + 1).start()

        @pl.when(t + o < n_t)
        def _():
            xcopy(1, o - 1, h, t + o, t).wait_recv()

            @pl.when(t > 0)
            def _():
                xcopy(1, o, h, t + o, t - 1).start()

    def far(j):
        wcopy(5, j, dp ^ 6, py, h=0).wait_recv()
        wcopy(6, j, dp ^ 6, px, h=1).wait_recv()
        wcopy(7, j, dp ^ 6, mate).start()

    def ready(j):
        far(j)
        wcopy(2, j, mate, mate).wait_recv()
        wcopy(3, j, dp ^ 3, mate).wait_recv()
        wcopy(4, j, dp ^ 5, mate).wait_recv()
        wcopy(7, j, dp ^ 7, mate).wait_recv()

    factor = query_scalar ** (-0.5)
    low = t < n_t // 2
    sign = jnp.where(low, 1, -1)
    m = jnp.where(low, t, n_t - 1 - t)
    fwd = jnp.where(low, 0, 1)

    def mirror(b):
        return jnp.where(low, b, n_t - 1 - b)

    places = (
        t,
        jnp.where(m == 0, t + sign, t - sign),
        jnp.where(m == 0, t + 2 * sign, t + sign),
        mirror(n_t - 1),
    )

    def head_cols(j, i):
        return pl.ds(pl.multiple_of(j * qw + i * hd, hd), hd)

    def tiles(*which):
        for slot, (j, p) in enumerate(which):
            here = pl.ds(pl.multiple_of(places[p] * rows, rows), rows)
            proj[slot] = lax.dot_general(x[here, :], w[j], NN, preferred_element_type=F32)
        for slot, (j, p) in enumerate(which):
            here = pl.ds(pl.multiple_of(places[p] * rows, rows), rows)
            cosv, sinv = cos_ref[...], sin_ref[...]

            def turn(v):
                return v * cosv + swap_halves(v) * sinv

            def unturn(v):
                return v * cosv - swap_halves(v) * sinv

            q = jnp.concatenate(
                [turn(proj[slot, :, i * hd : (i + 1) * hd]).astype(BF16) for i in range(rep)], 0
            )
            k = turn(proj[slot, :, qw : qw + hd]).astype(BF16)
            v = proj[slot, :, qw + hd : cw].astype(BF16)
            cot = jnp.concatenate(
                [cot_ref[here, head_cols(j, i)] for i in range(rep)], 0
            )
            bent = jnp.tanh(
                lax.dot_general(q, k, NT, preferred_element_type=F32) * factor / CAP
            )
            raised = jnp.exp(CAP * bent) * mask_ref[...]
            weights = raised / jnp.sum(raised, -1, keepdims=True)
            probs = weights.astype(BF16)
            att = lax.dot_general(probs, v, NN, preferred_element_type=F32).astype(BF16)
            d_probs = lax.dot_general(cot, v, NT, preferred_element_type=F32)
            d_capped = weights * (d_probs - jnp.sum(weights * d_probs, -1, keepdims=True))
            ds = (d_capped * (1.0 - bent * bent) * factor).astype(BF16)
            dq = lax.dot_general(ds, k, NN, preferred_element_type=F32)
            dk = lax.dot_general(ds, q, TN, preferred_element_type=F32)
            dv = lax.dot_general(probs, cot, TN, preferred_element_type=F32)
            for i in range(rep):
                part = slice(i * rows, (i + 1) * rows)
                att_ref[here, head_cols(j, i)] = att[part]
                dproj[j, here, i * hd : (i + 1) * hd] = unturn(dq[part]).astype(BF16)
            dproj[j, here, qw : qw + hd] = unturn(dk).astype(BF16)
            dproj[j, here, qw + hd : cw] = dv.astype(BF16)
    def zcopy(way, b, h, to):
        src = dn.at[pl.ds(pl.multiple_of(b * rows + h * piece, piece), piece)]
        return rdma(
            src,
            rb.at[way, b, pl.ds(h * piece, piece)],
            zs.at[way, b, h],
            zr.at[way, b, h],
            dp,
            to,
        )

    tile = 256

    def back(first, count):
        here = pl.ds(pl.multiple_of(first * rows, rows), count * rows)

        def cols(n, c2):
            span = pl.ds(pl.multiple_of(n * tile, tile), tile)
            total = lax.dot_general(
                dproj[0, here, :], w[0, span, :], NT, preferred_element_type=F32
            )
            for j in range(1, chunks):
                total += lax.dot_general(
                    dproj[j, here, :], w[j, span, :], NT, preferred_element_type=F32
                )
            dn[here, span] = total.astype(BF16)
            return c2

        lax.fori_loop(0, width // tile, cols, 0)

    def outward(b, halves=(0, 1)):
        for h in halves:
            zcopy(fwd, mirror(b), h, t + sign).start()

    def gcopy(kind, j, src, dst, to):
        return rdma(src, dst, gs.at[kind, j], gr.at[kind, j], to, t)

    def to_mate(j):
        return gcopy(0, j, g.at[j, :, 1 - core], pr.at[j], mate)

    lo, hi = pl.ds(0, half), pl.ds(half, half)
    cx, cy, cd = chip ^ 1, chip ^ 2, chip ^ 3

    def d_x(j):
        return gcopy(1, j, cs.at[j, cd, lo], dr.at[j, lo], px)

    def d_y(j):
        return gcopy(2, j, cs.at[j, cd, hi], dr.at[j, hi], py)

    def x_lo(j):
        return gcopy(3, j, cs.at[j, cx, lo], ar.at[0, j, lo], px)

    def x_hi(j):
        return gcopy(4, j, cs.at[j, cx, hi], ar.at[0, j, hi], px)

    def y_lo(j):
        return gcopy(5, j, cs.at[j, cy, lo], ar.at[1, j, lo], py)

    def y_hi(j):
        return gcopy(6, j, cs.at[j, cy, hi], ar.at[1, j, hi], py)

    def add(*parts):
        total = parts[0].astype(F32)
        for part in parts[1:]:
            total = total + part.astype(F32)
        return total.astype(BF16)

    def product(j):
        def share(c, c2):
            for k in range(2):
                span = pl.ds(pl.multiple_of((2 * c + k) * shard, 16), shard)
                g[j, c, k] = lax.dot_general(
                    xt[span, :], dproj[j], NN, preferred_element_type=F32
                ).astype(BF16)
            return c2

        lax.fori_loop(0, n_dp // 2, share, 0)
        to_mate(j).start()

    def on_chip(j):
        to_mate(j).wait_recv()
        for c in range(n_dp // 2):
            cs[j, c] = add(g[j, c, core], pr[j, c])
        d_x(j).start()
        d_y(j).start()
        x_lo(j).start()
        y_hi(j).start()

    def pass_on(j):
        d_x(j).wait_recv()
        cs[j, cy, lo] = add(cs[j, cy, lo], dr[j, lo])
        y_lo(j).start()
        d_y(j).wait_recv()
        cs[j, cx, hi] = add(cs[j, cx, hi], dr[j, hi])
        x_hi(j).start()

    def zsum(way, b, h):
        here = pl.ds(pl.multiple_of(b * rows + h * piece, piece), piece)
        zcopy(way, b, h, t).wait_recv()
        dn[here, :] = add(dn[here, :], rb[way, b, h * piece : (h + 1) * piece])

    far_block = mirror(n_t - 1)
    rest = jnp.where(low, 0, 1)

    relay(0)
    offer(2)
    xrelay(1, 0)
    relay(1)
    offer(3)
    xrelay(1, 1)
    ready(0)
    tiles((0, 0), (0, 1))
    xrelay(2, 0)
    relay(2)
    ready(1)
    xrelay(2, 1)
    tiles((1, 0), (1, 1))
    tiles((0, 2), (1, 2))
    relay(3)
    ready(2)
    tiles((2, 0), (2, 1), (2, 2))
    ready(3)
    xrelay(3, 0)
    xrelay(3, 1)
    tiles((0, 3), (1, 3))
    xt[...] = x[...].T
    product(0)
    tiles((2, 3), (3, 3))
    back(far_block, 1)

    @pl.when(m == 0)
    def _():
        outward(n_t - 1)

    on_chip(0)
    product(1)
    tiles((3, 0), (3, 1), (3, 2))
    back(rest, n_t - 1)

    @pl.when(m == 0)
    def _():
        outward(n_t - 2)
        outward(1)

    on_chip(1)
    product(2)

    @pl.when(m > 0)
    def _():
        for h in range(2):
            zsum(fwd, far_block, h)
            outward(n_t - 1, (h,))

    product(3)
    on_chip(2)
    pass_on(0)
    on_chip(3)
    pass_on(1)

    @pl.when(m > 0)
    def _():
        b = mirror(0)
        for h in range(2):
            zsum(1 - fwd, b, h)
            zcopy(1 - fwd, b, h, t - sign).start()
            zsum(fwd, mirror(n_t - 2), h)
            outward(n_t - 2, (h,))

    pass_on(2)
    pass_on(3)

    mine = pl.ds(pl.multiple_of(t * rows, rows), rows)
    for h in range(2):
        zcopy(1 - fwd, t, h, t).wait_recv()

    @pl.when(m > 0)
    def _():
        for h in range(2):
            zcopy(fwd, t, h, t).wait_recv()

    @pl.when(m == 0)
    def _():
        rb[fwd, t] = jnp.zeros((rows, width), BF16)

    d_normed = dn[mine, :].astype(F32) + rb[0, t].astype(F32) + rb[1, t].astype(F32)
    tokens2 = tok_ref[...].astype(F32)
    inv2 = lax.rsqrt(jnp.mean(tokens2 * tokens2, -1, keepdims=True) + EPS)
    unit = tokens2 * inv2
    pb1[dp] = jnp.sum(d_normed * unit, 0, keepdims=True)

    def p1(o):
        return rdma(pb1.at[dp], pb1.at[dp], ps.at[0, o], prs.at[0, o], dp ^ o, t)

    def p2(o):
        return rdma(pb2.at[t], pb2.at[t], ps.at[1, o], prs.at[1, o], dp, t ^ o)

    def p1r(o):
        return rdma(pb1.at[dp ^ o], pb1.at[dp ^ o], ps.at[0, o], prs.at[0, o], dp ^ o, t)

    def p2r(o):
        return rdma(pb2.at[t ^ o], pb2.at[t ^ o], ps.at[1, o], prs.at[1, o], dp, t ^ o)

    for o in range(1, n_dp):
        p1(o).start()
    e = d_normed * gain_ref[...][None, :]
    gtok_ref[...] = (inv2 * (e - unit * jnp.mean(e * unit, -1, keepdims=True))).astype(BF16)
    for o in range(1, n_dp):
        p1r(o).wait_recv()
    total = pb1[0]
    for o in range(1, n_dp):
        total = total + pb1[o]
    pb2[t] = total
    for o in range(1, n_t):
        p2(o).start()

    for j in range(chunks):
        x_lo(j).wait_recv()
        y_hi(j).wait_recv()
        y_lo(j).wait_recv()
        x_hi(j).wait_recv()
        done = add(cs[j, chip], ar[0, j], ar[1, j])
        gq_ref[:, j * qw : (j + 1) * qw] = done[:, :qw]
        gk_ref[:, j * hd : (j + 1) * hd] = done[:, qw : qw + hd]
        gv_ref[:, j * hd : (j + 1) * hd] = done[:, qw + hd :]

    for o in range(1, n_t):
        p2r(o).wait_recv()
    total = pb2[0]
    for o in range(1, n_t):
        total = total + pb2[o]
    gpre_ref[...] = total[0]

    for j in range(chunks):
        wcopy(0, j, dp, px).wait_send()
        wcopy(1, j, dp, py).wait_send()
        wcopy(2, j, dp, mate).wait_send()
        wcopy(3, j, px, mate).wait_send()
        wcopy(4, j, py, mate).wait_send()
        wcopy(5, j, px, py, h=0).wait_send()
        wcopy(6, j, py, px, h=1).wait_send()
        wcopy(7, j, dp ^ 6, mate).wait_send()
        to_mate(j).wait_send()
        for copy in (d_x, d_y, x_lo, x_hi, y_lo, y_hi):
            copy(j).wait_send()
    for h in range(2):
        for o in range(n_t - 1):
            @pl.when((t - o >= 0) & (t + 1 < n_t))
            def _():
                xcopy(0, o, h, t - o, t + 1).wait_send()

            @pl.when((t + o < n_t) & (t > 0))
            def _():
                xcopy(1, o, h, t + o, t - 1).wait_send()

        for b in range(n_t - 1, 0, -1):
            @pl.when(m < b)
            def _():
                zcopy(fwd, mirror(b), h, t + sign).wait_send()

        @pl.when(m > 0)
        def _():
            zcopy(1 - fwd, mirror(0), h, t - sign).wait_send()

    for o in range(1, n_dp):
        p1(o).wait_send()
    for o in range(1, n_t):
        p2(o).wait_send()


def fused_per_device(tokens, cotangent, pre_gain, w_query, key_weight, value_weight):
    n_dp, n_t = lax.axis_size("dp"), lax.axis_size("tensor")
    rows, width = tokens.shape
    block = rows * n_t
    shard = w_query.shape[0]
    chunks = key_weight.shape[1] // HEAD_SIZE
    rep = w_query.shape[1] // key_weight.shape[1]
    qw = rep * HEAD_SIZE
    cw = qw + 2 * HEAD_SIZE
    half = HEAD_SIZE // 2
    place = np.arange(rows)
    freqs = BASE ** (-np.arange(half) / half)
    angles = (place % SEQ_LEN)[:, None] * freqs[None, :]
    cosine = np.concatenate([np.cos(angles)] * 2, -1).astype(np.float32)
    sine = np.concatenate([-np.sin(angles), np.sin(angles)], -1).astype(np.float32)
    mask = (place[None, :] <= place[:, None]) & (
        place[None, :] // SEQ_LEN == place[:, None] // SEQ_LEN
    )
    mask = np.tile(mask.astype(np.float32), (rep, 1))
    vmem = pl.BlockSpec(memory_space=pltpu.VMEM)
    hbm = pl.BlockSpec(memory_space=pl.ANY)
    dma = pltpu.SemaphoreType.DMA
    attended, grad_tokens, gq, gk, gv, grad_pre = pl.pallas_call(
        functools.partial(whole_kernel, (n_dp, n_t, chunks, rep, HEAD_SIZE)),
        out_shape=(
            jax.ShapeDtypeStruct((block, chunks * qw), BF16),
            jax.ShapeDtypeStruct((rows, width), BF16),
            jax.ShapeDtypeStruct((shard, chunks * qw), BF16),
            jax.ShapeDtypeStruct((shard, chunks * HEAD_SIZE), BF16),
            jax.ShapeDtypeStruct((shard, chunks * HEAD_SIZE), BF16),
            jax.ShapeDtypeStruct((width,), F32),
        ),
        in_specs=[vmem, vmem, hbm, hbm, hbm] + [vmem] * 4,
        out_specs=(vmem,) * 6,
        scratch_shapes=[
            pltpu.VMEM((block, width), BF16),
            pltpu.VMEM((width, block), BF16),
            pltpu.VMEM((chunks, width, cw), BF16),
            pltpu.VMEM((3, rows, cw), F32),
            pltpu.VMEM((chunks, block, cw), BF16),
            pltpu.VMEM((chunks, n_dp // 2, 2, shard, cw), BF16),
            pltpu.VMEM((chunks, n_dp // 2, shard, cw), BF16),
            pltpu.VMEM((chunks, n_dp // 2, shard, cw), BF16),
            pltpu.VMEM((chunks, shard, cw), BF16),
            pltpu.VMEM((2, chunks, shard, cw), BF16),
            pltpu.VMEM((block, width), BF16),
            pltpu.VMEM((2, n_t, rows, width), BF16),
            pltpu.VMEM((n_dp, 1, width), F32),
            pltpu.VMEM((n_t, 1, width), F32),
            dma((8, chunks)),
            dma((8, chunks)),
            dma((2, n_t, 2)),
            dma((2, n_t, 2)),
            dma((7, chunks)),
            dma((7, chunks)),
            dma((2, n_t, 2)),
            dma((2, n_t, 2)),
            dma((2, n_dp)),
            dma((2, n_dp)),
            dma((3, chunks)),
        ],
        compiler_params=pltpu.CompilerParams(
            collective_id=0, has_side_effects=True, vmem_limit_bytes=62 * 1024 * 1024
        ),
    )(tokens, pre_gain, w_query, key_weight, value_weight, cotangent, cosine, sine, mask)
    return (
        attended,
        grad_tokens,
        gq.astype(F32),
        gk.astype(F32),
        gv.astype(F32),
        grad_pre,
    )


def solution(mesh):
    fused = mesh.shape["dp"] == 8 and mesh.shape["tensor"] == 4
    placed = (
        P(("dp", "tensor"), None),
        P("dp", "tensor"),
        P(),
        P("dp", "tensor"),
        P("dp", "tensor"),
        P("dp", "tensor"),
    )
    return jax.shard_map(
        fused_per_device if fused else per_device,
        mesh=mesh,
        in_specs=placed,
        out_specs=(
            P("dp", "tensor"),
            P(("dp", "tensor"), None),
            P("dp", "tensor"),
            P("dp", "tensor"),
            P("dp", "tensor"),
            P(),
        ),
        check_vma=False,
    )
```
